128 devices in a mesh: part: 1, data: 2 (over core), time: 64 (over z, y, x).
Axes of the slice: x: 4, y: 4, z: 4, core: 2. Of those that a mesh axis runs over, the one named last changes fastest.
Arguments:
- x_init: float32 [4, 4096, 16], P(('part', 'data'))
- w_in: bfloat16 [16, 1152], replicated
- w_out: bfloat16 [1152, 16], replicated
- mod_scale: bfloat16 [128, 1152], P('time')
- mod_shift: bfloat16 [128, 1152], P('time')
- step_size: float32 [128], P('time')
Outputs:
- output: float32 [128, 4, 4096, 16], P('time', ('part', 'data'))
All inputs are finite; a program needn't handle non-finite values.
Results may differ from the reference program's by a relative error of at most 0.001.
Values are sent between devices in bfloat16 or wider.
A program may use at most 1 GiB of HBM per device.

```python
import jax
import jax.numpy as jnp
from jax import lax

TOKENS = 4096
CHANNELS = 16
HIDDEN = 1152
STEPS = 128
BATCH = 4
SWEEPS = 4
HORIZON = 2


def setup_inputs(seed: int = 0, part: int = 0) -> dict:
    keys = jax.random.split(jax.random.key(seed), 8)
    x_init = jax.random.normal(jax.random.fold_in(keys[0], part), (BATCH, TOKENS, CHANNELS), jnp.float32)
    w_in = (jax.random.normal(keys[1], (CHANNELS, HIDDEN), jnp.float32) * CHANNELS ** -0.5).astype(jnp.bfloat16)
    w_out = (jax.random.normal(keys[2], (HIDDEN, CHANNELS), jnp.float32) * HIDDEN ** -0.5).astype(jnp.bfloat16)
    mod_scale = (0.5 * jax.random.normal(keys[3], (STEPS, HIDDEN), jnp.float32)).astype(jnp.bfloat16)
    mod_shift = (0.5 * jax.random.normal(keys[4], (STEPS, HIDDEN), jnp.float32)).astype(jnp.bfloat16)
    slope = jax.random.uniform(keys[5], (), jnp.float32, -3.0, 3.0)
    grid = (jnp.arange(STEPS, dtype=jnp.float32) + 0.5) / STEPS - 0.5
    weight = jnp.exp(slope * grid + 0.3 * jax.random.normal(keys[6], (STEPS,), jnp.float32))
    step_size = HORIZON * weight / jnp.sum(weight)
    return {"x_init": x_init, "w_in": w_in, "w_out": w_out, "mod_scale": mod_scale, "mod_shift": mod_shift, "step_size": step_size}


def reference(x_init, w_in, w_out, mod_scale, mod_shift, step_size):
    scale_one = 1.0 + mod_scale.astype(jnp.float32)
    shift_val = mod_shift.astype(jnp.float32)

    def drift_step(operands):
        latent, scale_row, shift_row, size_one = operands
        flat = latent.reshape(-1, latent.shape[-1]).astype(jnp.bfloat16)
        pre = jnp.dot(flat, w_in, preferred_element_type=jnp.float32)
        act = jax.nn.gelu(pre * scale_row + shift_row, approximate=True)
        out = jnp.dot(act.astype(jnp.bfloat16), w_out, preferred_element_type=jnp.float32)
        return (out * size_one).reshape(latent.shape)

    def one_sweep(latents, unused):
        drift = lax.map(drift_step, (latents, scale_one, shift_val, step_size))
        running = jnp.cumsum(drift, axis=0)
        preceding = jnp.concatenate([jnp.zeros_like(running[:1]), running[:-1]], axis=0)
        return x_init[None] + preceding, None

    start_lat = jnp.broadcast_to(x_init[None], (step_size.shape[0],) + x_init.shape)
    final, unused = lax.scan(one_sweep, start_lat, None, length=SWEEPS)
    return final
```

```python
import functools

import jax
import jax.numpy as jnp
from jax import lax
from jax.experimental import pallas as pl
from jax.experimental.pallas import tpu as pltpu
from jax.sharding import PartitionSpec as P

SWEEPS = 4
LIN = 2.0 * 0.7978845608028654
CUB = 8.0 * 0.7978845608028654 * 0.044715
LANES = 128
F32 = jnp.float32
BF16 = jnp.bfloat16


def kernel(n_time, x_hbm, w_in_ref, w_out_ref, scale_ref, shift_ref, step_ref, out_ref,
           x_own, w_in32, mods, steps, step_own, w3, w_all, rhs0, rhs_all, raw_all, stage, run_sum,
           pre0, pre1, act0, act1,
           local_sem, mod_send, mod_recv, step_send, step_recv, out_send, out_recv):
    hidden = w_in_ref.shape[1]
    chunks = hidden // 128
    tiles = x_hbm.shape[2] // LANES
    me = lax.axis_index("time")
    samp = me // tiles
    off = pl.multiple_of(lax.rem(me, tiles) * LANES, LANES)
    pres, acts = (pre0, pre1), (act0, act1)

    copies = [
        pltpu.make_async_copy(x_hbm.at[samp, :, pl.ds(off, LANES)], x_own, local_sem.at[0]),
        pltpu.make_async_copy(scale_ref, mods.at[me, 0], local_sem.at[1]),
        pltpu.make_async_copy(shift_ref, mods.at[me, 1], local_sem.at[2]),
    ]
    for c in copies:
        c.start()
    for a in range(2):
        step_own[a:a + 1, :] = jnp.full((1, LANES), step_ref[a], F32)
    w_in32[...] = w_in_ref[...].astype(F32)
    for c in copies:
        c.wait()

    def mod_copy(slot, peer):
        return pltpu.make_async_remote_copy(
            src_ref=mods.at[slot], dst_ref=mods.at[slot], send_sem=mod_send, recv_sem=mod_recv.at[slot],
            device_id={"time": peer}, device_id_type=pl.DeviceIdType.MESH)

    def step_copy(peer):
        return pltpu.make_async_remote_copy(
            src_ref=step_own, dst_ref=steps.at[me], send_sem=step_send, recv_sem=step_recv,
            device_id={"time": peer}, device_id_type=pl.DeviceIdType.MESH)

    def out_copy(pair):
        return pltpu.make_async_remote_copy(
            src_ref=stage.at[pair], dst_ref=out_ref.at[:, samp, :, pl.ds(off, LANES)],
            send_sem=out_send, recv_sem=out_recv,
            device_id={"time": pair}, device_id_type=pl.DeviceIdType.MESH)

    def send_out(pair):
        @pl.when(pair != me)
        def _():
            out_copy(pair).start()

    own_step = pltpu.make_async_copy(step_own, steps.at[me], local_sem.at[0])
    own_step.start()

    @pl.loop(1, n_time)
    def _(r):
        mod_copy(me, lax.rem(me + n_time - r, n_time)).start()

    @pl.loop(1, n_time)
    def _(r):
        step_copy(lax.rem(me + n_time - r, n_time)).start()

    x_bf = x_own[...].astype(BF16)
    one_row = jnp.where(lax.broadcasted_iota(jnp.int32, (16, LANES), 0) == 0, 1.0, 0.0).astype(BF16)
    zero_blk = jnp.zeros((64, LANES), BF16)

    def fill_const(ref):
        for a in range(2):
            ref[64 * a:64 * a + 64, LANES * (1 - a):LANES * (2 - a)] = zero_blk
            ref[64 * a + 48:64 * a + 64, LANES * a:LANES * (a + 1)] = one_row

    def fill_x(ref, a, val):
        for m in range(3):
            ref[64 * a + 16 * m:64 * a + 16 * m + 16, LANES * a:LANES * (a + 1)] = val

    fill_const(rhs0)
    for a in range(2):
        fill_x(rhs0, a, x_bf)

    first_row = lax.broadcasted_iota(jnp.int32, (16, hidden), 0) == 0

    def prep(pair):
        for a in range(2):
            s = 0.5 * (1.0 + mods[pair, 0, a:a + 1, :].astype(F32))
            b = 0.5 * mods[pair, 1, a:a + 1, :].astype(F32)
            p = w_in32[...] * s
            for m in range(3):
                q = p.astype(BF16)
                w3[64 * a + 16 * m:64 * a + 16 * m + 16, :] = q
                if m < 2:
                    p = p - q.astype(F32)
            w3[64 * a + 48:64 * a + 64, :] = jnp.where(first_row, b, 0.0).astype(BF16)
        for c in range(chunks):
            w_all[pair, 128 * c:128 * c + 128, :] = w3[:, 128 * c:128 * c + 128].T

    def body(a_pair, b_on, c_on, par, rhs=None):
        pre_w, pre_r, act_w, act_r = pres[par], pres[1 - par], acts[1 - par], acts[par]
        total = None
        if a_pair is not None and rhs is None:
            rhs = rhs_all.at[a_pair]
        for c in range(chunks):
            rows = slice(128 * c, 128 * c + 128)
            if c_on and c % 2 == 0:
                k_rows = slice(128 * c, min(128 * c + 256, hidden))
                part = jnp.dot(w_out_ref[:, k_rows], act_r[k_rows, :], preferred_element_type=F32)
                total = part if total is None else total + part
            if a_pair is not None:
                pre_w[rows, :] = jnp.dot(w_all[a_pair, rows, :], rhs[...], preferred_element_type=F32)
            if b_on:
                for k in range(8):
                    sub = slice(128 * c + 16 * k, 128 * c + 16 * k + 16)
                    h = pre_r[sub, :]
                    t = jnp.tanh(h * (LIN + CUB * (h * h)))
                    act_w[sub, :] = (h + h * t).astype(BF16)
        return total

    def drift_to_x(pair, raw, emit):
        total = jnp.where(pair == 0, 0.0, run_sum[...])
        for a in range(2):
            emit(a, x_own[...] + total)
            total = total + raw[:, LANES * a:LANES * (a + 1)] * steps[pair, a:a + 1, :]
        run_sum[...] = total

    def emit_rhs(pair):
        def emit(a, val):
            fill_x(rhs_all.at[pair], a, val.astype(BF16))
        return emit

    def emit_stage(pair):
        def emit(a, val):
            stage[pair, a] = val
        return emit

    def rot(i):
        return lax.rem(me + i, n_time)

    prep(me)
    mod_copy(rot(1), me).wait_recv()
    prep(rot(1))
    body(rot(0), False, False, 0, rhs0)

    def first(t, par):
        mod_copy(rot(t + 1), me).wait_recv()
        prep(rot(t + 1))
        fill_const(rhs_all.at[t])
        raw = body(rot(t), True, True, par, rhs0)
        raw_all[rot(t - 2)] = raw

    mod_copy(rot(2), me).wait_recv()
    prep(rot(2))
    fill_const(rhs_all.at[0])
    fill_const(rhs_all.at[1])
    body(rot(1), True, False, 1, rhs0)

    @pl.loop(0, (n_time - 4) // 2)
    def _(i):
        first(2 * i + 2, 0)
        first(2 * i + 3, 1)

    first(n_time - 2, 0)
    fill_const(rhs_all.at[n_time - 1])
    raw_all[rot(n_time - 3)] = body(rot(n_time - 1), True, True, 1, rhs0)
    raw_all[rot(n_time - 2)] = body(None, True, True, 0)
    raw_all[rot(n_time - 1)] = body(None, False, True, 1)

    others = pl.ds(0, n_time - 1)
    own_step.wait()
    pltpu.make_async_copy(steps.at[others], steps.at[others], step_recv).wait()

    def spread(pair):
        drift_to_x(pair, raw_all[pair], emit_rhs(pair))

    def mid(t, par, first_sweep):
        c_pair = lax.rem(t - 2, n_time)
        raw = body(lax.rem(t, n_time), True, True, par)
        return c_pair, raw

    @pl.loop(0, n_time // 4)
    def _(i):
        for k in range(4):
            spread(4 * i + k)

    body(0, False, False, 0)
    body(1, True, False, 1)

    @pl.loop(0, (SWEEPS - 2) * n_time // 2)
    def _(i):
        for par in range(2):
            c_pair, raw = mid(2 * i + 2 + par, par, False)
            drift_to_x(c_pair, raw, emit_rhs(c_pair))

    @pl.loop(0, (n_time - 2) // 2)
    def _(i):
        for par in range(2):
            pair = 2 * i + par
            if par == 0:
                @pl.when(i > 0)
                def _():
                    send_out(pair - 1)
            else:
                send_out(pair - 1)
            raw = body(pair + 2, True, True, par)
            drift_to_x(pair, raw, emit_stage(pair))

    send_out(n_time - 3)
    drift_to_x(n_time - 2, body(None, True, True, 0), emit_stage(n_time - 2))
    send_out(n_time - 2)
    drift_to_x(n_time - 1, body(None, False, True, 1), emit_stage(n_time - 1))
    send_out(n_time - 1)

    own_out = pltpu.make_async_copy(stage.at[me], out_ref.at[:, samp, :, pl.ds(off, LANES)], local_sem.at[0])
    own_out.start()
    own_out.wait()
    for ref, sem in ((stage, out_send), (mods, mod_send), (steps, step_send), (stage, out_recv)):
        pltpu.make_async_copy(ref.at[others], ref.at[others], sem).wait()


def solution(mesh):
    n_time = mesh.shape["time"]

    def local_run(x_init, w_in, w_out, mod_scale, mod_shift, step_size):
        x_t = jnp.transpose(x_init, (0, 2, 1))
        chan, hidden = w_in.shape
        batch, tokens = x_init.shape[0], x_init.shape[1]
        vmem = pl.BlockSpec(memory_space=pltpu.VMEM)
        out = pl.pallas_call(
            functools.partial(kernel, n_time),
            out_shape=jax.ShapeDtypeStruct((2, batch, chan, tokens), F32),
            in_specs=[pl.BlockSpec(memory_space=pl.ANY), vmem, vmem, vmem, vmem,
                      pl.BlockSpec(memory_space=pltpu.SMEM)],
            out_specs=vmem,
            scratch_shapes=[
                pltpu.VMEM((chan, LANES), F32),
                pltpu.VMEM((chan, hidden), F32),
                pltpu.VMEM((n_time, 2, 2, hidden), BF16),
                pltpu.VMEM((n_time, 2, LANES), F32),
                pltpu.VMEM((2, LANES), F32),
                pltpu.VMEM((128, hidden), BF16),
                pltpu.VMEM((n_time, hidden, 128), BF16),
                pltpu.VMEM((128, 2 * LANES), BF16),
                pltpu.VMEM((n_time, 128, 2 * LANES), BF16),
                pltpu.VMEM((n_time, chan, 2 * LANES), F32),
                pltpu.VMEM((n_time, 2, chan, LANES), F32),
                pltpu.VMEM((chan, LANES), F32),
                pltpu.VMEM((hidden, 2 * LANES), F32),
                pltpu.VMEM((hidden, 2 * LANES), F32),
                pltpu.VMEM((hidden, 2 * LANES), BF16),
                pltpu.VMEM((hidden, 2 * LANES), BF16),
                pltpu.SemaphoreType.DMA((3,)),
                pltpu.SemaphoreType.DMA,
                pltpu.SemaphoreType.DMA((n_time,)),
                pltpu.SemaphoreType.DMA,
                pltpu.SemaphoreType.DMA,
                pltpu.SemaphoreType.DMA,
                pltpu.SemaphoreType.DMA,
            ],
            compiler_params=pltpu.CompilerParams(has_side_effects=True, vmem_limit_bytes=58 * 1024 * 1024),
            name="picard",
        )(x_t, w_in, w_out.T, mod_scale, mod_shift, step_size)
        return jnp.transpose(out, (0, 1, 3, 2))

    return jax.shard_map(
        local_run,
        mesh=mesh,
        in_specs=(P(("part", "data"), None, None), P(None, None), P(None, None), P("time", None), P("time", None), P("time")),
        out_specs=P("time", ("part", "data"), None, None),
        check_vma=False,
    )
```

```python
import functools

import jax
import jax.numpy as jnp
from jax import lax
from jax.experimental import pallas as pl
from jax.experimental.pallas import tpu as pltpu
from jax.sharding import PartitionSpec as P

SWEEPS = 4
LIN = 2.0 * 0.7978845608028654
CUB = 8.0 * 0.7978845608028654 * 0.044715
LANES = 128
F32 = jnp.float32
BF16 = jnp.bfloat16


def kernel(n_time, x_hbm, w_in_ref, w_out_ref, scale_ref, shift_ref, step_ref, out_ref,
           x_own, w_in32, mods, steps, step_own, w_all, rhs0, rhs_all, raw_all, stage, run_sum,
           pre0, pre1, act0, act1, wp0, wp1,
           local_sem, mod_send, mod_recv, step_send, step_recv, out_send, out_recv):
    hidden = w_in_ref.shape[1]
    chunks = hidden // 128
    tiles = x_hbm.shape[2] // LANES
    me = lax.axis_index("time")
    samp = me // tiles
    off = pl.multiple_of(lax.rem(me, tiles) * LANES, LANES)
    pres, acts, wps = (pre0, pre1), (act0, act1), (wp0, wp1)

    copies = [
        pltpu.make_async_copy(x_hbm.at[samp, :, pl.ds(off, LANES)], x_own, local_sem.at[0]),
        pltpu.make_async_copy(scale_ref, mods.at[me, 0], local_sem.at[1]),
        pltpu.make_async_copy(shift_ref, mods.at[me, 1], local_sem.at[2]),
    ]
    for c in copies:
        c.start()
    for a in range(2):
        step_own[a:a + 1, :] = jnp.full((1, LANES), step_ref[a], F32)
    w_in32[...] = w_in_ref[...].astype(F32)
    for c in copies:
        c.wait()

    def mod_copy(slot, peer):
        return pltpu.make_async_remote_copy(
            src_ref=mods.at[slot], dst_ref=mods.at[slot], send_sem=mod_send, recv_sem=mod_recv.at[slot],
            device_id={"time": peer}, device_id_type=pl.DeviceIdType.MESH)

    def step_copy(peer):
        return pltpu.make_async_remote_copy(
            src_ref=step_own, dst_ref=steps.at[me], send_sem=step_send, recv_sem=step_recv,
            device_id={"time": peer}, device_id_type=pl.DeviceIdType.MESH)

    def out_copy(pair):
        return pltpu.make_async_remote_copy(
            src_ref=stage.at[pair], dst_ref=out_ref.at[:, samp, :, pl.ds(off, LANES)],
            send_sem=out_send, recv_sem=out_recv,
            device_id={"time": pair}, device_id_type=pl.DeviceIdType.MESH)

    def send_out(pair):
        @pl.when(pair != me)
        def _():
            out_copy(pair).start()

    own_step = pltpu.make_async_copy(step_own, steps.at[me], local_sem.at[0])
    own_step.start()

    @pl.loop(1, n_time)
    def _(r):
        mod_copy(me, lax.rem(me + n_time - r, n_time)).start()

    @pl.loop(1, n_time)
    def _(r):
        step_copy(lax.rem(me + n_time - r, n_time)).start()

    x_bf = x_own[...].astype(BF16)
    one_row = jnp.where(lax.broadcasted_iota(jnp.int32, (16, LANES), 0) == 0, 1.0, 0.0).astype(BF16)
    zero_blk = jnp.zeros((64, LANES), BF16)

    def fill_const(ref):
        for a in range(2):
            ref[64 * a:64 * a + 64, LANES * (1 - a):LANES * (2 - a)] = zero_blk
            ref[64 * a + 48:64 * a + 64, LANES * a:LANES * (a + 1)] = one_row

    def fill_x(ref, a, val):
        for m in range(3):
            ref[64 * a + 16 * m:64 * a + 16 * m + 16, LANES * a:LANES * (a + 1)] = val

    fill_const(rhs0)
    for a in range(2):
        fill_x(rhs0, a, x_bf)

    first_row = lax.broadcasted_iota(jnp.int32, (16, 128), 0) == 0

    def prep(pair, c, w_ref):
        cols = slice(128 * c, 128 * c + 128)
        blocks = []
        for a in range(2):
            s = 0.5 * (1.0 + mods[pair, 0, a:a + 1, cols].astype(F32))
            b = 0.5 * mods[pair, 1, a:a + 1, cols].astype(F32)
            p = w_in32[:, cols] * s
            for m in range(3):
                q = p.astype(BF16)
                blocks.append(q)
                if m < 2:
                    p = p - q.astype(F32)
            blocks.append(jnp.where(first_row, b, 0.0).astype(BF16))
        w_t = jnp.concatenate(blocks, axis=0).T
        w_ref[cols, :] = w_t
        w_all[pair, cols, :] = w_t

    def body(a_pair, b_on, c_on, par, rhs=None, nxt=None):
        pre_w, pre_r, act_w, act_r = pres[par], pres[1 - par], acts[1 - par], acts[par]
        total = None
        if a_pair is not None:
            w = w_all.at[a_pair] if rhs is None else wps[par]
            rhs = rhs_all.at[a_pair] if rhs is None else rhs
        for c in range(chunks):
            rows = slice(128 * c, 128 * c + 128)
            if c_on and c % 2 == 0:
                k_rows = slice(128 * c, min(128 * c + 256, hidden))
                part = jnp.dot(w_out_ref[:, k_rows], act_r[k_rows, :], preferred_element_type=F32)
                total = part if total is None else total + part
            if a_pair is not None:
                pre_w[rows, :] = jnp.dot(w[rows, :], rhs[...], preferred_element_type=F32)
            if nxt is not None:
                prep(nxt, c, wps[1 - par])
            if b_on:
                for k in range(8):
                    sub = slice(128 * c + 16 * k, 128 * c + 16 * k + 16)
                    h = pre_r[sub, :]
                    t = jnp.tanh(h * (LIN + CUB * (h * h)))
                    act_w[sub, :] = (h + h * t).astype(BF16)
        return total

    def drift_to_x(pair, raw, emit):
        total = jnp.where(pair == 0, 0.0, run_sum[...])
        for a in range(2):
            emit(a, x_own[...] + total)
            total = total + raw[:, LANES * a:LANES * (a + 1)] * steps[pair, a:a + 1, :]
        run_sum[...] = total

    def emit_rhs(pair):
        def emit(a, val):
            fill_x(rhs_all.at[pair], a, val.astype(BF16))
        return emit

    def emit_stage(pair):
        def emit(a, val):
            stage[pair, a] = val
        return emit

    def rot(i):
        return lax.rem(me + i, n_time)

    for c in range(chunks):
        prep(me, c, wps[0])
    mod_copy(rot(1), me).wait_recv()
    body(rot(0), False, False, 0, rhs0, rot(1))
    mod_copy(rot(2), me).wait_recv()
    body(rot(1), True, False, 1, rhs0, rot(2))
    fill_const(rhs_all.at[0])
    fill_const(rhs_all.at[1])

    def first(t, par):
        raw_all[rot(t - 2)] = body(rot(t), True, True, par, rhs0, rot(t + 1))
        fill_const(rhs_all.at[t])

    @pl.loop(0, (n_time - 4) // 2)
    def _(i):
        t = 2 * i + 2
        mod_copy(rot(t + 1), me).wait_recv()
        mod_copy(rot(t + 2), me).wait_recv()
        first(t, 0)
        first(t + 1, 1)

    mod_copy(rot(n_time - 1), me).wait_recv()
    first(n_time - 2, 0)
    raw_all[rot(n_time - 3)] = body(rot(n_time - 1), True, True, 1, rhs0)
    fill_const(rhs_all.at[n_time - 1])
    raw_all[rot(n_time - 2)] = body(None, True, True, 0)
    raw_all[rot(n_time - 1)] = body(None, False, True, 1)

    others = pl.ds(0, n_time - 1)
    own_step.wait()
    pltpu.make_async_copy(steps.at[others], steps.at[others], step_recv).wait()

    def spread(pair):
        drift_to_x(pair, raw_all[pair], emit_rhs(pair))

    @pl.loop(0, n_time // 4)
    def _(i):
        for k in range(4):
            spread(4 * i + k)

    body(0, False, False, 0)
    body(1, True, False, 1)

    @pl.loop(0, (SWEEPS - 2) * n_time // 2)
    def _(i):
        t = 2 * i + 2
        raws = [body(lax.rem(t + par, n_time), True, True, par) for par in range(2)]
        for par in range(2):
            pair = lax.rem(2 * i + par, n_time)
            drift_to_x(pair, raws[par], emit_rhs(pair))

    @pl.loop(0, (n_time - 2) // 2)
    def _(i):
        for par in range(2):
            pair = 2 * i + par
            if par == 0:
                @pl.when(i > 0)
                def _():
                    send_out(pair - 1)
            else:
                send_out(pair - 1)
            raw = body(pair + 2, True, True, par)
            drift_to_x(pair, raw, emit_stage(pair))

    send_out(n_time - 3)
    drift_to_x(n_time - 2, body(None, True, True, 0), emit_stage(n_time - 2))
    send_out(n_time - 2)
    drift_to_x(n_time - 1, body(None, False, True, 1), emit_stage(n_time - 1))
    send_out(n_time - 1)

    own_out = pltpu.make_async_copy(stage.at[me], out_ref.at[:, samp, :, pl.ds(off, LANES)], local_sem.at[0])
    own_out.start()
    own_out.wait()
    for ref, sem in ((stage, out_send), (mods, mod_send), (steps, step_send), (stage, out_recv)):
        pltpu.make_async_copy(ref.at[others], ref.at[others], sem).wait()


def solution(mesh):
    n_time = mesh.shape["time"]

    def local_run(x_init, w_in, w_out, mod_scale, mod_shift, step_size):
        x_t = jnp.transpose(x_init, (0, 2, 1))
        chan, hidden = w_in.shape
        batch, tokens = x_init.shape[0], x_init.shape[1]
        vmem = pl.BlockSpec(memory_space=pltpu.VMEM)
        out = pl.pallas_call(
            functools.partial(kernel, n_time),
            out_shape=jax.ShapeDtypeStruct((2, batch, chan, tokens), F32),
            in_specs=[pl.BlockSpec(memory_space=pl.ANY), vmem, vmem, vmem, vmem,
                      pl.BlockSpec(memory_space=pltpu.SMEM)],
            out_specs=vmem,
            scratch_shapes=[
                pltpu.VMEM((chan, LANES), F32),
                pltpu.VMEM((chan, hidden), F32),
                pltpu.VMEM((n_time, 2, 2, hidden), BF16),
                pltpu.VMEM((n_time, 2, LANES), F32),
                pltpu.VMEM((2, LANES), F32),
                pltpu.VMEM((n_time, hidden, 128), BF16),
                pltpu.VMEM((128, 2 * LANES), BF16),
                pltpu.VMEM((n_time, 128, 2 * LANES), BF16),
                pltpu.VMEM((n_time, chan, 2 * LANES), F32),
                pltpu.VMEM((n_time, 2, chan, LANES), F32),
                pltpu.VMEM((chan, LANES), F32),
                pltpu.VMEM((hidden, 2 * LANES), F32),
                pltpu.VMEM((hidden, 2 * LANES), F32),
                pltpu.VMEM((hidden, 2 * LANES), BF16),
                pltpu.VMEM((hidden, 2 * LANES), BF16),
                pltpu.VMEM((hidden, 128), BF16),
                pltpu.VMEM((hidden, 128), BF16),
                pltpu.SemaphoreType.DMA((3,)),
                pltpu.SemaphoreType.DMA,
                pltpu.SemaphoreType.DMA((n_time,)),
                pltpu.SemaphoreType.DMA,
                pltpu.SemaphoreType.DMA,
                pltpu.SemaphoreType.DMA,
                pltpu.SemaphoreType.DMA,
            ],
            compiler_params=pltpu.CompilerParams(has_side_effects=True, vmem_limit_bytes=58 * 1024 * 1024),
            name="picard",
        )(x_t, w_in, w_out.T, mod_scale, mod_shift, step_size)
        return jnp.transpose(out, (0, 1, 3, 2))

    return jax.shard_map(
        local_run,
        mesh=mesh,
        in_specs=(P(("part", "data"), None, None), P(None, None), P(None, None), P("time", None), P("time", None), P("time")),
        out_specs=P("time", ("part", "data"), None, None),
        check_vma=False,
    )
```

```python
import functools

import jax
import jax.numpy as jnp
from jax import lax
from jax.experimental import pallas as pl
from jax.experimental.pallas import tpu as pltpu
from jax.sharding import PartitionSpec as P

SWEEPS = 4
AHEAD = 16
LIN = 2.0 * 0.7978845608028654
CUB = 8.0 * 0.7978845608028654 * 0.044715
LANES = 128
F32 = jnp.float32
BF16 = jnp.bfloat16


def kernel(n_time, x_hbm, w_in_ref, w_out_ref, scale_ref, shift_ref, step_ref, out_ref, fix_ref,
           x_own, w_in32, mods, steps, step_own, w_all, rhs0, rhs_all, raw_all, stage, fix, run_sum,
           pre0, pre1, act0, act1, wp0, wp1,
           local_sem, mod_send, mod_recv, step_send, step_recv, out_send, out_recv, fix_send, fix_recv):
    hidden = w_in_ref.shape[1]
    chunks = hidden // 128
    tiles = x_hbm.shape[2] // LANES
    me = lax.axis_index("time")
    samp = me // tiles
    off = pl.multiple_of(lax.rem(me, tiles) * LANES, LANES)
    pres, acts, wps = (pre0, pre1), (act0, act1), (wp0, wp1)

    copies = [
        pltpu.make_async_copy(x_hbm.at[samp, :, pl.ds(off, LANES)], x_own, local_sem.at[0]),
        pltpu.make_async_copy(scale_ref, mods.at[me, 0], local_sem.at[1]),
        pltpu.make_async_copy(shift_ref, mods.at[me, 1], local_sem.at[2]),
    ]
    for c in copies:
        c.start()
    for a in range(2):
        step_own[a:a + 1, :] = jnp.full((1, LANES), step_ref[a], F32)
    w_in32[...] = w_in_ref[...].astype(F32)
    for c in copies:
        c.wait()

    def mod_copy(slot, peer):
        return pltpu.make_async_remote_copy(
            src_ref=mods.at[slot], dst_ref=mods.at[slot], send_sem=mod_send, recv_sem=mod_recv.at[slot],
            device_id={"time": peer}, device_id_type=pl.DeviceIdType.MESH)

    def step_copy(peer):
        return pltpu.make_async_remote_copy(
            src_ref=step_own, dst_ref=steps.at[me], send_sem=step_send, recv_sem=step_recv,
            device_id={"time": peer}, device_id_type=pl.DeviceIdType.MESH)

    def send_to(pair, src, dst, send, recv):
        @pl.when(pair != me)
        def _():
            pltpu.make_async_remote_copy(
                src_ref=src.at[pair], dst_ref=dst.at[:, samp, :, pl.ds(off, LANES)], send_sem=send, recv_sem=recv,
                device_id={"time": pair}, device_id_type=pl.DeviceIdType.MESH).start()

    def send_base(pair):
        send_to(pair, stage, out_ref, out_send, out_recv)

    def send_fix(pair):
        send_to(pair, fix, fix_ref, fix_send, fix_recv)

    own_step = pltpu.make_async_copy(step_own, steps.at[me], local_sem.at[0])
    own_step.start()

    def send_mods(r):
        peer = lax.rem(me + n_time - r, n_time)
        mod_copy(me, peer).start()
        step_copy(peer).start()

    @pl.loop(1, AHEAD + 1)
    def _(r):
        send_mods(r)

    x_bf = x_own[...].astype(BF16)
    one_row = jnp.where(lax.broadcasted_iota(jnp.int32, (16, LANES), 0) == 0, 1.0, 0.0).astype(BF16)
    zero_blk = jnp.zeros((64, LANES), BF16)

    def fill_const(ref):
        for a in range(2):
            ref[64 * a:64 * a + 64, LANES * (1 - a):LANES * (2 - a)] = zero_blk
            ref[64 * a + 48:64 * a + 64, LANES * a:LANES * (a + 1)] = one_row

    def fill_x(ref, a, val):
        for m in range(3):
            ref[64 * a + 16 * m:64 * a + 16 * m + 16, LANES * a:LANES * (a + 1)] = val

    fill_const(rhs0)
    for a in range(2):
        fill_x(rhs0, a, x_bf)

    first_row = lax.broadcasted_iota(jnp.int32, (16, 128), 0) == 0

    def prep(pair, c, w_ref):
        cols = slice(128 * c, 128 * c + 128)
        blocks = []
        for a in range(2):
            s = 0.5 * (1.0 + mods[pair, 0, a:a + 1, cols].astype(F32))
            b = 0.5 * mods[pair, 1, a:a + 1, cols].astype(F32)
            p = w_in32[:, cols] * s
            for m in range(3):
                q = p.astype(BF16)
                blocks.append(q)
                if m < 2:
                    p = p - q.astype(F32)
            blocks.append(jnp.where(first_row, b, 0.0).astype(BF16))
        w_t = jnp.concatenate(blocks, axis=0).T
        w_ref[cols, :] = w_t
        w_all[pair, cols, :] = w_t

    def body(a_pair, b_on, c_on, par, rhs=None, nxt=None):
        pre_w, pre_r, act_w, act_r = pres[par], pres[1 - par], acts[1 - par], acts[par]
        total = None
        if a_pair is not None:
            w = w_all.at[a_pair] if rhs is None else wps[par]
            rhs = rhs_all.at[a_pair] if rhs is None else rhs
        for c in range(chunks):
            rows = slice(128 * c, 128 * c + 128)
            if c_on and c % 2 == 0:
                k_rows = slice(128 * c, min(128 * c + 256, hidden))
                part = jnp.dot(w_out_ref[:, k_rows], act_r[k_rows, :], preferred_element_type=F32)
                total = part if total is None else total + part
            if a_pair is not None:
                pre_w[rows, :] = jnp.dot(w[rows, :], rhs[...], preferred_element_type=F32)
            if nxt is not None:
                prep(nxt, c, wps[1 - par])
            if b_on:
                for k in range(8):
                    sub = slice(128 * c + 16 * k, 128 * c + 16 * k + 16)
                    h = pre_r[sub, :]
                    t = jnp.tanh(h * (LIN + CUB * (h * h)))
                    act_w[sub, :] = (h + h * t).astype(BF16)
        return total

    def drift_to_x(pair, raw, emit):
        total = jnp.where(pair == 0, 0.0, run_sum[...])
        for a in range(2):
            emit(a, x_own[...] + total)
            total = total + raw[:, LANES * a:LANES * (a + 1)] * steps[pair, a:a + 1, :]
        run_sum[...] = total

    def emit_rhs(pair):
        def emit(a, val):
            stage[pair, a] = val
            fill_x(rhs_all.at[pair], a, val.astype(BF16))
        return emit

    def emit_fix(pair):
        def emit(a, val):
            fix[pair, a] = (val - stage[pair, a]).astype(BF16)
        return emit

    def rot(i):
        return lax.rem(me + i, n_time)

    for c in range(chunks):
        prep(me, c, wps[0])
    mod_copy(rot(1), me).wait_recv()
    body(rot(0), False, False, 0, rhs0, rot(1))
    mod_copy(rot(2), me).wait_recv()
    body(rot(1), True, False, 1, rhs0, rot(2))
    fill_const(rhs_all.at[0])
    fill_const(rhs_all.at[1])

    def first(t, par):
        raw_all[rot(t - 2)] = body(rot(t), True, True, par, rhs0, rot(t + 1))
        fill_const(rhs_all.at[t])

    @pl.loop(0, (n_time - 4) // 2)
    def _(i):
        for par in range(2):
            t = 2 * i + 2 + par

            @pl.when(t - 1 + AHEAD < n_time)
            def _():
                send_mods(t - 1 + AHEAD)
            mod_copy(rot(t + 1), me).wait_recv()
            first(t, par)

    mod_copy(rot(n_time - 1), me).wait_recv()
    first(n_time - 2, 0)
    raw_all[rot(n_time - 3)] = body(rot(n_time - 1), True, True, 1, rhs0)
    fill_const(rhs_all.at[n_time - 1])
    raw_all[rot(n_time - 2)] = body(None, True, True, 0)
    raw_all[rot(n_time - 1)] = body(None, False, True, 1)

    others = pl.ds(0, n_time - 1)
    own_step.wait()
    pltpu.make_async_copy(steps.at[others], steps.at[others], step_recv).wait()

    def spread(pair):
        drift_to_x(pair, raw_all[pair], emit_rhs(pair))

    @pl.loop(0, n_time // 4)
    def _(i):
        for k in range(4):
            spread(4 * i + k)

    body(0, False, False, 0)
    body(1, True, False, 1)

    @pl.loop(0, (SWEEPS - 2) * n_time // 2)
    def _(i):
        for par in range(2):
            step = 2 * i + par
            pair = lax.rem(step, n_time)

            @pl.when(step >= (SWEEPS - 3) * n_time + 2)
            def _():
                send_base(pair - 2)
            raw = body(lax.rem(step + 2, n_time), True, True, par)
            drift_to_x(pair, raw, emit_rhs(pair))

    @pl.loop(0, (n_time - 2) // 2)
    def _(i):
        for par in range(2):
            pair = 2 * i + par

            @pl.when(i > 0)
            def _():
                send_fix(pair - 2)

            @pl.when(i == 0)
            def _():
                send_base(n_time - 2 + par)
            raw = body(pair + 2, True, True, par)
            drift_to_x(pair, raw, emit_fix(pair))

    send_fix(n_time - 4)
    send_fix(n_time - 3)
    drift_to_x(n_time - 2, body(None, True, True, 0), emit_fix(n_time - 2))
    send_fix(n_time - 2)
    drift_to_x(n_time - 1, body(None, False, True, 1), emit_fix(n_time - 1))
    send_fix(n_time - 1)

    own = [
        pltpu.make_async_copy(stage.at[me], out_ref.at[:, samp, :, pl.ds(off, LANES)], local_sem.at[0]),
        pltpu.make_async_copy(fix.at[me], fix_ref.at[:, samp, :, pl.ds(off, LANES)], local_sem.at[1]),
    ]
    for c in own:
        c.start()
    for ref, sem in ((mods, mod_send), (steps, step_send), (stage, out_send), (fix, fix_send), (stage, out_recv), (fix, fix_recv)):
        pltpu.make_async_copy(ref.at[others], ref.at[others], sem).wait()
    for c in own:
        c.wait()


def solution(mesh):
    n_time = mesh.shape["time"]

    def local_run(x_init, w_in, w_out, mod_scale, mod_shift, step_size):
        x_t = jnp.transpose(x_init, (0, 2, 1))
        chan, hidden = w_in.shape
        batch, tokens = x_init.shape[0], x_init.shape[1]
        vmem = pl.BlockSpec(memory_space=pltpu.VMEM)
        base, fix = pl.pallas_call(
            functools.partial(kernel, n_time),
            out_shape=[jax.ShapeDtypeStruct((2, batch, chan, tokens), t) for t in (F32, BF16)],
            in_specs=[pl.BlockSpec(memory_space=pl.ANY), vmem, vmem, vmem, vmem,
                      pl.BlockSpec(memory_space=pltpu.SMEM)],
            out_specs=[vmem, vmem],
            scratch_shapes=[
                pltpu.VMEM((chan, LANES), F32),
                pltpu.VMEM((chan, hidden), F32),
                pltpu.VMEM((n_time, 2, 2, hidden), BF16),
                pltpu.VMEM((n_time, 2, LANES), F32),
                pltpu.VMEM((2, LANES), F32),
                pltpu.VMEM((n_time, hidden, 128), BF16),
                pltpu.VMEM((128, 2 * LANES), BF16),
                pltpu.VMEM((n_time, 128, 2 * LANES), BF16),
                pltpu.VMEM((n_time, chan, 2 * LANES), F32),
                pltpu.VMEM((n_time, 2, chan, LANES), F32),
                pltpu.VMEM((n_time, 2, chan, LANES), BF16),
                pltpu.VMEM((chan, LANES), F32),
                pltpu.VMEM((hidden, 2 * LANES), F32),
                pltpu.VMEM((hidden, 2 * LANES), F32),
                pltpu.VMEM((hidden, 2 * LANES), BF16),
                pltpu.VMEM((hidden, 2 * LANES), BF16),
                pltpu.VMEM((hidden, 128), BF16),
                pltpu.VMEM((hidden, 128), BF16),
                pltpu.SemaphoreType.DMA((3,)),
                pltpu.SemaphoreType.DMA,
                pltpu.SemaphoreType.DMA((n_time,)),
                pltpu.SemaphoreType.DMA,
                pltpu.SemaphoreType.DMA,
                pltpu.SemaphoreType.DMA,
                pltpu.SemaphoreType.DMA,
                pltpu.SemaphoreType.DMA,
                pltpu.SemaphoreType.DMA,
            ],
            compiler_params=pltpu.CompilerParams(has_side_effects=True, vmem_limit_bytes=58 * 1024 * 1024),
            name="picard",
        )(x_t, w_in, w_out.T, mod_scale, mod_shift, step_size)
        return jnp.transpose(base + fix.astype(F32), (0, 1, 3, 2))

    return jax.shard_map(
        local_run,
        mesh=mesh,
        in_specs=(P(("part", "data"), None, None), P(None, None), P(None, None), P("time", None), P("time", None), P("time")),
        out_specs=P("time", ("part", "data"), None, None),
        check_vma=False,
    )
```

```python
import functools

import jax
import jax.numpy as jnp
from jax import lax
from jax.experimental import pallas as pl
from jax.experimental.pallas import tpu as pltpu
from jax.sharding import PartitionSpec as P

SWEEPS = 4
UNROLL = 8
LIN = 2.0 * 0.7978845608028654
CUB = 8.0 * 0.7978845608028654 * 0.044715
LANES = 128
F32 = jnp.float32
BF16 = jnp.bfloat16


def kernel(n_time, x_hbm, w_in_ref, w_out_ref, scale_ref, shift_ref, step_ref, out_ref, fix_ref,
           x_own, w_in32, mods, steps, step_own, w_all, rhs0, rhs_all, raw_all, raw_blk, stage, fix, run_sum,
           pre0, pre1, act0, act1, wp0, wp1,
           local_sem, mod_send, mod_recv, step_send, step_recv, out_send, out_recv, fix_send, fix_recv):
    hidden = w_in_ref.shape[1]
    chunks = hidden // 128
    tiles = x_hbm.shape[2] // LANES
    me = lax.axis_index("time")
    samp = me // tiles
    off = pl.multiple_of(lax.rem(me, tiles) * LANES, LANES)
    pres, acts, wps = (pre0, pre1), (act0, act1), (wp0, wp1)

    copies = [
        pltpu.make_async_copy(x_hbm.at[samp, :, pl.ds(off, LANES)], x_own, local_sem.at[0]),
        pltpu.make_async_copy(scale_ref, mods.at[me, 0], local_sem.at[1]),
        pltpu.make_async_copy(shift_ref, mods.at[me, 1], local_sem.at[2]),
    ]
    for c in copies:
        c.start()
    for a in range(2):
        step_own[a:a + 1, :] = jnp.full((1, LANES), step_ref[a], F32)
    w_in32[...] = w_in_ref[...].astype(F32)
    for c in copies:
        c.wait()

    def mod_copy(slot, peer):
        return pltpu.make_async_remote_copy(
            src_ref=mods.at[slot], dst_ref=mods.at[slot], send_sem=mod_send, recv_sem=mod_recv.at[slot],
            device_id={"time": peer}, device_id_type=pl.DeviceIdType.MESH)

    def step_copy(peer):
        return pltpu.make_async_remote_copy(
            src_ref=step_own, dst_ref=steps.at[me], send_sem=step_send, recv_sem=step_recv,
            device_id={"time": peer}, device_id_type=pl.DeviceIdType.MESH)

    def send_to(pair, src, dst, send, recv):
        @pl.when(pair != me)
        def _():
            pltpu.make_async_remote_copy(
                src_ref=src.at[pair], dst_ref=dst.at[:, samp, :, pl.ds(off, LANES)], send_sem=send, recv_sem=recv,
                device_id={"time": pair}, device_id_type=pl.DeviceIdType.MESH).start()

    def send_base(pair):
        send_to(pair, stage, out_ref, out_send, out_recv)

    def send_fix(pair):
        send_to(pair, fix, fix_ref, fix_send, fix_recv)

    own_step = pltpu.make_async_copy(step_own, steps.at[me], local_sem.at[0])
    own_step.start()

    def send_mods(r):
        peer = lax.rem(me + n_time - r, n_time)
        mod_copy(me, peer).start()
        step_copy(peer).start()

    @pl.loop(1, 3 * UNROLL + 1)
    def _(r):
        send_mods(r)

    x_bf = x_own[...].astype(BF16)
    one_row = jnp.where(lax.broadcasted_iota(jnp.int32, (16, LANES), 0) == 0, 1.0, 0.0).astype(BF16)
    zero_blk = jnp.zeros((64, LANES), BF16)

    def fill_const(ref):
        for a in range(2):
            ref[64 * a:64 * a + 64, LANES * (1 - a):LANES * (2 - a)] = zero_blk
            ref[64 * a + 48:64 * a + 64, LANES * a:LANES * (a + 1)] = one_row

    def fill_x(ref, a, val):
        for m in range(3):
            ref[64 * a + 16 * m:64 * a + 16 * m + 16, LANES * a:LANES * (a + 1)] = val

    fill_const(rhs0)
    for a in range(2):
        fill_x(rhs0, a, x_bf)

    first_row = lax.broadcasted_iota(jnp.int32, (16, hidden), 0) == 0

    def prep(pair, w_ref):
        blocks = []
        for a in range(2):
            s = 0.5 * (1.0 + mods[pair, 0, a:a + 1, :].astype(F32))
            b = 0.5 * mods[pair, 1, a:a + 1, :].astype(F32)
            p = w_in32[...] * s
            for m in range(3):
                q = p.astype(BF16)
                blocks.append(q)
                if m < 2:
                    p = p - q.astype(F32)
            blocks.append(jnp.where(first_row, b, 0.0).astype(BF16))
        w_t = jnp.concatenate(blocks, axis=0).T
        w_ref[...] = w_t
        w_all[pair] = w_t

    def body(a_pair, b_on, c_on, par, rhs=None, nxt=None):
        pre_w, pre_r, act_w, act_r = pres[par], pres[1 - par], acts[1 - par], acts[par]
        total = None
        if a_pair is not None:
            w = w_all.at[a_pair] if rhs is None else wps[par]
            rhs = rhs_all.at[a_pair] if rhs is None else rhs
        if a_pair is not None:
            pre_w[...] = jnp.dot(w[...], rhs[...], preferred_element_type=F32)
        if c_on:
            total = jnp.dot(w_out_ref[...], act_r[...], preferred_element_type=F32)
        if nxt is not None:
            prep(nxt, wps[1 - par])
        if b_on:
            for c in range(chunks):
                rows = slice(128 * c, 128 * c + 128)
                h = pre_r[rows, :]
                t = jnp.tanh(h * (LIN + CUB * (h * h)))
                act_w[rows, :] = (h + h * t).astype(BF16)
        return total

    def drift_to_x(pair, raw, emit):
        total = jnp.where(pair == 0, 0.0, run_sum[...])
        for a in range(2):
            emit(a, x_own[...] + total)
            total = total + raw[:, LANES * a:LANES * (a + 1)] * steps[pair, a:a + 1, :]
        run_sum[...] = total

    def emit_rhs(pair):
        def emit(a, val):
            stage[pair, a] = val
            fill_x(rhs_all.at[pair], a, val.astype(BF16))
        return emit

    def emit_fix(pair):
        def emit(a, val):
            fix[pair, a] = (val - stage[pair, a]).astype(BF16)
        return emit

    def rot(i):
        return lax.rem(me + i, n_time)

    def wait_mods(lo, count):
        for k in range(count):
            mod_copy(rot(lo + k), me).wait_recv()

    def block(lo, hi, f):
        @pl.loop(lo // 2, hi // 2, unroll=True)
        def _(kk):
            for par in range(2):
                f(2 * kk + par, par)

    def first(t, par, b_on=True, c_on=True, nxt=True):
        raw = body(rot(t), b_on, c_on, par, rhs0, rot(t + 1) if nxt else None)
        if c_on:
            raw_all[rot(t - 2)] = raw
        fill_const(rhs_all.at[t])

    prep(me, wps[0])
    wait_mods(1, 2)
    first(0, 0, False, False)
    first(1, 1, True, False)
    wait_mods(3, UNROLL - 2)
    block(2, UNROLL, first)

    @pl.loop(1, n_time // UNROLL - 1)
    def _(i):
        for k in range(UNROLL):
            r = UNROLL * (i + 2) + 1 + k

            @pl.when(r < n_time)
            def _():
                send_mods(r)
        wait_mods(UNROLL * i + 1, UNROLL)
        block(0, UNROLL, lambda k, par: first(UNROLL * i + k, par))

    wait_mods(n_time - UNROLL + 1, UNROLL - 1)
    block(n_time - UNROLL, n_time - 2, first)
    first(n_time - 2, 0)
    first(n_time - 1, 1, nxt=False)
    raw_all[rot(n_time - 2)] = body(None, True, True, 0)
    raw_all[rot(n_time - 1)] = body(None, False, True, 1)

    others = pl.ds(0, n_time - 1)
    own_step.wait()
    pltpu.make_async_copy(steps.at[others], steps.at[others], step_recv).wait()

    @pl.loop(0, n_time // 2 - 1)
    def _(i):
        for k in range(2):
            drift_to_x(2 * i + k, raw_all[2 * i + k], emit_rhs(2 * i + k))

    def finish_block(i):
        @pl.loop(0, UNROLL, unroll=True)
        def _(k):
            pair = lax.rem(UNROLL * i + k - 2 + n_time, n_time)
            drift_to_x(pair, raw_blk[k], emit_rhs(pair))

    per = n_time // UNROLL
    base_from = (SWEEPS - 3) * n_time

    def mid(k, par, t=None):
        raw_blk[k] = body(k if t is None else t, True, True, par)

    for k in range(2):
        raw_blk[k] = raw_all[n_time - 2 + k]
        body(k, k >= 1, False, k)
    block(2, UNROLL, mid)

    @pl.loop(1, (SWEEPS - 2) * per)
    def _(i):
        for k in range(UNROLL):
            step = UNROLL * (i - 2) + k - 2

            @pl.when(step >= base_from)
            def _():
                send_base(step - base_from)
        finish_block(i - 1)
        block(0, UNROLL, lambda k, par: mid(k, par, lax.rem(UNROLL * i + k, n_time)))

    @pl.loop(0, UNROLL)
    def _(k):
        send_base(n_time - 2 * UNROLL - 2 + k)
    finish_block((SWEEPS - 2) * per - 1)
    for k in range(2):
        drift_to_x(n_time - 2 + k, body(k, True, True, k), emit_rhs(n_time - 2 + k))

    def late(t, par):
        drift_to_x(t - 2, body(t, True, True, par), emit_fix(t - 2))

    block(2, UNROLL, late)

    @pl.loop(0, UNROLL + 2)
    def _(k):
        send_base(n_time - UNROLL - 2 + k)

    @pl.loop(0, UNROLL - 2)
    def _(k):
        send_fix(k)

    @pl.loop(1, per)
    def _(i):
        for k in range(UNROLL):
            @pl.when(i > 1)
            def _():
                send_fix(UNROLL * (i - 1) + k - 2)
        block(0, UNROLL, lambda k, par: late(UNROLL * i + k, par))

    @pl.loop(0, UNROLL)
    def _(k):
        send_fix(n_time - UNROLL - 2 + k)
    drift_to_x(n_time - 2, body(None, True, True, 0), emit_fix(n_time - 2))
    send_fix(n_time - 2)
    drift_to_x(n_time - 1, body(None, False, True, 1), emit_fix(n_time - 1))
    send_fix(n_time - 1)

    own = [
        pltpu.make_async_copy(stage.at[me], out_ref.at[:, samp, :, pl.ds(off, LANES)], local_sem.at[0]),
        pltpu.make_async_copy(fix.at[me], fix_ref.at[:, samp, :, pl.ds(off, LANES)], local_sem.at[1]),
    ]
    for c in own:
        c.start()
    for ref, sem in ((mods, mod_send), (steps, step_send), (stage, out_send), (fix, fix_send), (stage, out_recv), (fix, fix_recv)):
        pltpu.make_async_copy(ref.at[others], ref.at[others], sem).wait()
    for c in own:
        c.wait()


def solution(mesh):
    n_time = mesh.shape["time"]

    def local_run(x_init, w_in, w_out, mod_scale, mod_shift, step_size):
        x_t = jnp.transpose(x_init, (0, 2, 1))
        chan, hidden = w_in.shape
        batch, tokens = x_init.shape[0], x_init.shape[1]
        vmem = pl.BlockSpec(memory_space=pltpu.VMEM)
        base, fix = pl.pallas_call(
            functools.partial(kernel, n_time),
            out_shape=[jax.ShapeDtypeStruct((2, batch, chan, tokens), t) for t in (F32, BF16)],
            in_specs=[pl.BlockSpec(memory_space=pl.ANY), vmem, vmem, vmem, vmem,
                      pl.BlockSpec(memory_space=pltpu.SMEM)],
            out_specs=[vmem, vmem],
            scratch_shapes=[
                pltpu.VMEM((chan, LANES), F32),
                pltpu.VMEM((chan, hidden), F32),
                pltpu.VMEM((n_time, 2, 2, hidden), BF16),
                pltpu.VMEM((n_time, 2, LANES), F32),
                pltpu.VMEM((2, LANES), F32),
                pltpu.VMEM((n_time, hidden, 128), BF16),
                pltpu.VMEM((128, 2 * LANES), BF16),
                pltpu.VMEM((n_time, 128, 2 * LANES), BF16),
                pltpu.VMEM((n_time, chan, 2 * LANES), F32),
                pltpu.VMEM((UNROLL, chan, 2 * LANES), F32),
                pltpu.VMEM((n_time, 2, chan, LANES), F32),
                pltpu.VMEM((n_time, 2, chan, LANES), BF16),
                pltpu.VMEM((chan, LANES), F32),
                pltpu.VMEM((hidden, 2 * LANES), F32),
                pltpu.VMEM((hidden, 2 * LANES), F32),
                pltpu.VMEM((hidden, 2 * LANES), BF16),
                pltpu.VMEM((hidden, 2 * LANES), BF16),
                pltpu.VMEM((hidden, 128), BF16),
                pltpu.VMEM((hidden, 128), BF16),
                pltpu.SemaphoreType.DMA((3,)),
                pltpu.SemaphoreType.DMA,
                pltpu.SemaphoreType.DMA((n_time,)),
                pltpu.SemaphoreType.DMA,
                pltpu.SemaphoreType.DMA,
                pltpu.SemaphoreType.DMA,
                pltpu.SemaphoreType.DMA,
                pltpu.SemaphoreType.DMA,
                pltpu.SemaphoreType.DMA,
            ],
            compiler_params=pltpu.CompilerParams(has_side_effects=True, vmem_limit_bytes=58 * 1024 * 1024),
            name="picard",
        )(x_t, w_in, w_out.T, mod_scale, mod_shift, step_size)
        return jnp.transpose(base + fix.astype(F32), (0, 1, 3, 2))

    return jax.shard_map(
        local_run,
        mesh=mesh,
        in_specs=(P(("part", "data"), None, None), P(None, None), P(None, None), P("time", None), P("time", None), P("time")),
        out_specs=P("time", ("part", "data"), None, None),
        check_vma=False,
    )
```

```python
import functools

import jax
import jax.numpy as jnp
from jax import lax
from jax.experimental import pallas as pl
from jax.experimental.pallas import tpu as pltpu
from jax.sharding import PartitionSpec as P

SWEEPS = 4
UNROLL = 8
ROOT = 0.7978845608028654
CUBE = (ROOT * 0.044715) ** (1.0 / 3.0)
LIN = ROOT / CUBE
LANES = 128
F32 = jnp.float32
BF16 = jnp.bfloat16


def kernel(n_time, x_hbm, w_in_ref, w_out_ref, scale_ref, shift_ref, step_ref, out_ref, fix_ref,
           x_own, w_in32, mods, steps, step_own, w_all, rhs0, rhs_all, raw_all, raw_blk, stage, fix, run_sum,
           pre0, pre1, act0, act1, wp0, wp1, w_out3,
           local_sem, mod_send, mod_recv, step_send, step_recv, out_send, out_recv, fix_send, fix_recv):
    hidden = w_in_ref.shape[1]
    chunks = hidden // 128
    tiles = x_hbm.shape[2] // LANES
    me = lax.axis_index("time")
    samp = me // tiles
    off = pl.multiple_of(lax.rem(me, tiles) * LANES, LANES)
    pres, acts, wps = (pre0, pre1), (act0, act1), (wp0, wp1)

    copies = [
        pltpu.make_async_copy(x_hbm.at[samp, :, pl.ds(off, LANES)], x_own, local_sem.at[0]),
        pltpu.make_async_copy(scale_ref, mods.at[me, 0], local_sem.at[1]),
        pltpu.make_async_copy(shift_ref, mods.at[me, 1], local_sem.at[2]),
    ]
    for c in copies:
        c.start()
    for a in range(2):
        step_own[a:a + 1, :] = jnp.full((1, LANES), step_ref[a], F32)
    w_in32[...] = w_in_ref[...].astype(F32)
    for c in copies:
        c.wait()

    def mod_copy(slot, peer):
        return pltpu.make_async_remote_copy(
            src_ref=mods.at[slot], dst_ref=mods.at[slot], send_sem=mod_send, recv_sem=mod_recv.at[slot],
            device_id={"time": peer}, device_id_type=pl.DeviceIdType.MESH)

    def step_copy(peer):
        return pltpu.make_async_remote_copy(
            src_ref=step_own, dst_ref=steps.at[me], send_sem=step_send, recv_sem=step_recv,
            device_id={"time": peer}, device_id_type=pl.DeviceIdType.MESH)

    def send_to(pair, src, dst, send, recv):
        @pl.when(pair != me)
        def _():
            pltpu.make_async_remote_copy(
                src_ref=src.at[pair], dst_ref=dst.at[:, samp, :, pl.ds(off, LANES)], send_sem=send, recv_sem=recv,
                device_id={"time": pair}, device_id_type=pl.DeviceIdType.MESH).start()

    def send_base(pair):
        send_to(pair, stage, out_ref, out_send, out_recv)

    def send_fix(pair):
        send_to(pair, fix, fix_ref, fix_send, fix_recv)

    own_step = pltpu.make_async_copy(step_own, steps.at[me], local_sem.at[0])
    own_step.start()

    def send_mods(r):
        peer = lax.rem(me + n_time - r, n_time)
        mod_copy(me, peer).start()
        step_copy(peer).start()

    @pl.loop(1, 3 * UNROLL + 1)
    def _(r):
        send_mods(r)

    x_bf = x_own[...].astype(BF16)
    one_row = jnp.where(lax.broadcasted_iota(jnp.int32, (16, LANES), 0) < 3, 1.0, 0.0).astype(BF16)
    zero_blk = jnp.zeros((64, LANES), BF16)

    def fill_const(ref):
        for a in range(2):
            ref[64 * a:64 * a + 64, LANES * (1 - a):LANES * (2 - a)] = zero_blk
            ref[64 * a + 48:64 * a + 64, LANES * a:LANES * (a + 1)] = one_row

    def fill_x(ref, a, val):
        for m in range(3):
            ref[64 * a + 16 * m:64 * a + 16 * m + 16, LANES * a:LANES * (a + 1)] = val

    fill_const(rhs0)
    for a in range(2):
        fill_x(rhs0, a, x_bf)

    row_of = lax.broadcasted_iota(jnp.int32, (8, hidden), 0)

    def terms(p):
        out = []
        for m in range(3):
            out.append(p.astype(BF16))
            if m < 2:
                p = p - out[m].astype(F32)
        return out

    w_out3[...] = jnp.concatenate(terms(w_out_ref[...].astype(F32) * (0.5 / CUBE)), axis=0)

    def prep(pair, w_ref):
        blocks = []
        for a in range(2):
            blocks += terms(w_in32[...] * (CUBE * (1.0 + mods[pair, 0, a:a + 1, :].astype(F32))))
            b = CUBE * mods[pair, 1, a:a + 1, :].astype(F32)
            rows = jnp.zeros((8, hidden), F32)
            for m, q in enumerate(terms(b)):
                rows = jnp.where(row_of == m, q.astype(F32), rows)
            blocks.append(jnp.concatenate([rows, jnp.zeros((8, hidden), F32)], axis=0).astype(BF16))
        w_t = jnp.concatenate(blocks, axis=0).T
        w_ref[...] = w_t
        w_all[pair] = w_t

    def body(a_pair, b_on, c_on, par, rhs=None, nxt=None):
        pre_w, pre_r, act_w, act_r = pres[par], pres[1 - par], acts[1 - par], acts[par]
        total = None
        if a_pair is not None:
            w = w_all.at[a_pair] if rhs is None else wps[par]
            rhs = rhs_all.at[a_pair] if rhs is None else rhs
        if a_pair is not None:
            pre_w[...] = jnp.dot(w[...], rhs[...], preferred_element_type=F32)
        if c_on:
            parts = jnp.dot(w_out3[...], act_r[...], preferred_element_type=F32)
            total = parts[:16] + (parts[16:32] + parts[32:])
        if nxt is not None:
            prep(nxt, wps[1 - par])
        if b_on:
            for c in range(chunks):
                rows = slice(128 * c, 128 * c + 128)
                h = pre_r[rows, :]
                t = jnp.tanh(h * (LIN + h * h))
                act_w[rows, :] = (h + h * t).astype(BF16)
        return total

    def drift_to_x(pair, raw, emit):
        total = jnp.where(pair == 0, 0.0, run_sum[...])
        for a in range(2):
            emit(a, x_own[...] + total)
            total = total + raw[:, LANES * a:LANES * (a + 1)] * steps[pair, a:a + 1, :]
        run_sum[...] = total

    def emit_rhs(pair):
        def emit(a, val):
            stage[pair, a] = val
            fill_x(rhs_all.at[pair], a, val.astype(BF16))
        return emit

    def emit_fix(pair):
        def emit(a, val):
            fix[pair, a] = (val - stage[pair, a]).astype(BF16)
        return emit

    def rot(i):
        return lax.rem(me + i, n_time)

    def wait_mods(lo, count):
        for k in range(count):
            mod_copy(rot(lo + k), me).wait_recv()

    def block(lo, hi, f):
        @pl.loop(lo // 2, hi // 2, unroll=True)
        def _(kk):
            for par in range(2):
                f(2 * kk + par, par)

    def first(t, par, b_on=True, c_on=True, nxt=True):
        raw = body(rot(t), b_on, c_on, par, rhs0, rot(t + 1) if nxt else None)
        if c_on:
            raw_all[rot(t - 2)] = raw
        fill_const(rhs_all.at[t])

    prep(me, wps[0])
    wait_mods(1, 2)
    first(0, 0, False, False)
    first(1, 1, True, False)
    wait_mods(3, UNROLL - 2)
    block(2, UNROLL, first)

    @pl.loop(1, n_time // UNROLL - 1)
    def _(i):
        for k in range(UNROLL):
            r = UNROLL * (i + 2) + 1 + k

            @pl.when(r < n_time)
            def _():
                send_mods(r)
        wait_mods(UNROLL * i + 1, UNROLL)
        block(0, UNROLL, lambda k, par: first(UNROLL * i + k, par))

    wait_mods(n_time - UNROLL + 1, UNROLL - 1)
    block(n_time - UNROLL, n_time - 2, first)
    first(n_time - 2, 0)
    first(n_time - 1, 1, nxt=False)
    raw_all[rot(n_time - 2)] = body(None, True, True, 0)
    raw_all[rot(n_time - 1)] = body(None, False, True, 1)

    others = pl.ds(0, n_time - 1)
    own_step.wait()
    pltpu.make_async_copy(steps.at[others], steps.at[others], step_recv).wait()

    @pl.loop(0, n_time // 2 - 1)
    def _(i):
        for k in range(2):
            drift_to_x(2 * i + k, raw_all[2 * i + k], emit_rhs(2 * i + k))

    def finish_block(i):
        @pl.loop(0, UNROLL, unroll=True)
        def _(k):
            pair = lax.rem(UNROLL * i + k - 2 + n_time, n_time)
            drift_to_x(pair, raw_blk[k], emit_rhs(pair))

    per = n_time // UNROLL
    base_from = (SWEEPS - 3) * n_time

    def mid(k, par, t=None):
        raw_blk[k] = body(k if t is None else t, True, True, par)

    for k in range(2):
        raw_blk[k] = raw_all[n_time - 2 + k]
        body(k, k >= 1, False, k)
    block(2, UNROLL, mid)

    @pl.loop(1, (SWEEPS - 2) * per)
    def _(i):
        for k in range(UNROLL):
            step = UNROLL * (i - 2) + k - 2

            @pl.when(step >= base_from)
            def _():
                send_base(step - base_from)
        finish_block(i - 1)
        block(0, UNROLL, lambda k, par: mid(k, par, lax.rem(UNROLL * i + k, n_time)))

    @pl.loop(0, UNROLL)
    def _(k):
        send_base(n_time - 2 * UNROLL - 2 + k)
    finish_block((SWEEPS - 2) * per - 1)
    for k in range(2):
        drift_to_x(n_time - 2 + k, body(k, True, True, k), emit_rhs(n_time - 2 + k))

    def late(t, par):
        drift_to_x(t - 2, body(t, True, True, par), emit_fix(t - 2))

    block(2, UNROLL, late)

    @pl.loop(0, UNROLL + 2)
    def _(k):
        send_base(n_time - UNROLL - 2 + k)

    @pl.loop(0, UNROLL - 2)
    def _(k):
        send_fix(k)

    @pl.loop(1, per - 1)
    def _(i):
        for k in range(UNROLL):
            @pl.when(i > 1)
            def _():
                send_fix(UNROLL * (i - 1) + k - 2)
        block(0, UNROLL, lambda k, par: late(UNROLL * i + k, par))

    @pl.loop(0, UNROLL)
    def _(k):
        send_fix(n_time - 2 * UNROLL - 2 + k)

    @pl.loop(n_time // 2 - UNROLL // 2, n_time // 2)
    def _(i):
        for par in range(2):
            late(2 * i + par, par)
        for par in range(2):
            send_fix(2 * i + par - 2)

    drift_to_x(n_time - 2, body(None, True, True, 0), emit_fix(n_time - 2))
    send_fix(n_time - 2)
    drift_to_x(n_time - 1, body(None, False, True, 1), emit_fix(n_time - 1))
    send_fix(n_time - 1)

    own = [
        pltpu.make_async_copy(stage.at[me], out_ref.at[:, samp, :, pl.ds(off, LANES)], local_sem.at[0]),
        pltpu.make_async_copy(fix.at[me], fix_ref.at[:, samp, :, pl.ds(off, LANES)], local_sem.at[1]),
    ]
    for c in own:
        c.start()
    for ref, sem in ((mods, mod_send), (steps, step_send), (stage, out_send), (fix, fix_send), (stage, out_recv), (fix, fix_recv)):
        pltpu.make_async_copy(ref.at[others], ref.at[others], sem).wait()
    for c in own:
        c.wait()


def solution(mesh):
    n_time = mesh.shape["time"]

    def local_run(x_init, w_in, w_out, mod_scale, mod_shift, step_size):
        x_t = jnp.transpose(x_init, (0, 2, 1))
        chan, hidden = w_in.shape
        batch, tokens = x_init.shape[0], x_init.shape[1]
        vmem = pl.BlockSpec(memory_space=pltpu.VMEM)
        base, fix = pl.pallas_call(
            functools.partial(kernel, n_time),
            out_shape=[jax.ShapeDtypeStruct((2, batch, chan, tokens), t) for t in (F32, BF16)],
            in_specs=[pl.BlockSpec(memory_space=pl.ANY), vmem, vmem, vmem, vmem,
                      pl.BlockSpec(memory_space=pltpu.SMEM)],
            out_specs=[vmem, vmem],
            scratch_shapes=[
                pltpu.VMEM((chan, LANES), F32),
                pltpu.VMEM((chan, hidden), F32),
                pltpu.VMEM((n_time, 2, 2, hidden), BF16),
                pltpu.VMEM((n_time, 2, LANES), F32),
                pltpu.VMEM((2, LANES), F32),
                pltpu.VMEM((n_time, hidden, 128), BF16),
                pltpu.VMEM((128, 2 * LANES), BF16),
                pltpu.VMEM((n_time, 128, 2 * LANES), BF16),
                pltpu.VMEM((n_time, chan, 2 * LANES), F32),
                pltpu.VMEM((UNROLL, chan, 2 * LANES), F32),
                pltpu.VMEM((n_time, 2, chan, LANES), F32),
                pltpu.VMEM((n_time, 2, chan, LANES), BF16),
                pltpu.VMEM((chan, LANES), F32),
                pltpu.VMEM((hidden, 2 * LANES), F32),
                pltpu.VMEM((hidden, 2 * LANES), F32),
                pltpu.VMEM((hidden, 2 * LANES), BF16),
                pltpu.VMEM((hidden, 2 * LANES), BF16),
                pltpu.VMEM((hidden, 128), BF16),
                pltpu.VMEM((hidden, 128), BF16),
                pltpu.VMEM((3 * chan, hidden), BF16),
                pltpu.SemaphoreType.DMA((3,)),
                pltpu.SemaphoreType.DMA,
                pltpu.SemaphoreType.DMA((n_time,)),
                pltpu.SemaphoreType.DMA,
                pltpu.SemaphoreType.DMA,
                pltpu.SemaphoreType.DMA,
                pltpu.SemaphoreType.DMA,
                pltpu.SemaphoreType.DMA,
                pltpu.SemaphoreType.DMA,
            ],
            compiler_params=pltpu.CompilerParams(has_side_effects=True, vmem_limit_bytes=58 * 1024 * 1024),
            name="picard",
        )(x_t, w_in, w_out.T, mod_scale, mod_shift, step_size)
        return jnp.transpose(base + fix.astype(F32), (0, 1, 3, 2))

    return jax.shard_map(
        local_run,
        mesh=mesh,
        in_specs=(P(("part", "data"), None, None), P(None, None), P(None, None), P("time", None), P("time", None), P("time")),
        out_specs=P("time", ("part", "data"), None, None),
        check_vma=False,
    )
```

```python
import functools

import jax
import jax.numpy as jnp
from jax import lax
from jax.experimental import pallas as pl
from jax.experimental.pallas import tpu as pltpu
from jax.sharding import PartitionSpec as P

SWEEPS = 4
UNROLL = 8
ROOT = 0.7978845608028654
CUBE = (ROOT * 0.044715) ** (1.0 / 3.0)
LIN = ROOT / CUBE
LANES = 128
F32 = jnp.float32
BF16 = jnp.bfloat16


def kernel(n_time, x_hbm, w_in_ref, w_out_ref, scale_ref, shift_ref, step_ref, out_ref, fix_ref,
           x_own, w_in32, mods, steps, step_own, w_all, rhs0, rhs_all, raw_all, raw_blk, stage, fix, run_sum,
           pre0, pre1, act0, act1, wp0, wp1, w_out3,
           local_sem, mod_send, mod_recv, step_send, step_recv, out_send, out_recv, fix_send, fix_recv):
    hidden = w_in_ref.shape[1]
    chunks = hidden // 128
    tiles = x_hbm.shape[2] // LANES
    me = lax.axis_index("time")
    samp = me // tiles
    off = pl.multiple_of(lax.rem(me, tiles) * LANES, LANES)
    pres, acts, wps = (pre0, pre1), (act0, act1), (wp0, wp1)

    barrier = pltpu.get_barrier_semaphore()

    @pl.loop(1, n_time)
    def _(r):
        pl.semaphore_signal(
            barrier, inc=1, device_id={"time": lax.rem(me + r, n_time)}, device_id_type=pl.DeviceIdType.MESH)

    copies = [
        pltpu.make_async_copy(x_hbm.at[samp, :, pl.ds(off, LANES)], x_own, local_sem.at[0]),
        pltpu.make_async_copy(scale_ref, mods.at[me, 0], local_sem.at[1]),
        pltpu.make_async_copy(shift_ref, mods.at[me, 1], local_sem.at[2]),
    ]
    for c in copies:
        c.start()
    for a in range(2):
        step_own[a:a + 1, :] = jnp.full((1, LANES), step_ref[a], F32)
    w_in32[...] = w_in_ref[...].astype(F32)
    for c in copies:
        c.wait()

    def mod_copy(slot, peer):
        return pltpu.make_async_remote_copy(
            src_ref=mods.at[slot], dst_ref=mods.at[slot], send_sem=mod_send, recv_sem=mod_recv.at[slot],
            device_id={"time": peer}, device_id_type=pl.DeviceIdType.MESH)

    def step_copy(peer):
        return pltpu.make_async_remote_copy(
            src_ref=step_own, dst_ref=steps.at[me], send_sem=step_send, recv_sem=step_recv,
            device_id={"time": peer}, device_id_type=pl.DeviceIdType.MESH)

    def send_to(pair, src, dst, send, recv):
        @pl.when(pair != me)
        def _():
            pltpu.make_async_remote_copy(
                src_ref=src.at[pair], dst_ref=dst.at[:, samp, :, pl.ds(off, LANES)], send_sem=send, recv_sem=recv,
                device_id={"time": pair}, device_id_type=pl.DeviceIdType.MESH).start()

    def send_base(pair):
        send_to(pair, stage, out_ref, out_send, out_recv)

    def send_fix(pair):
        send_to(pair, fix, fix_ref, fix_send, fix_recv)

    own_step = pltpu.make_async_copy(step_own, steps.at[me], local_sem.at[0])
    own_step.start()

    def send_mods(r):
        mod_copy(me, lax.rem(me + n_time - r, n_time)).start()

    x_bf = x_own[...].astype(BF16)
    one_row = jnp.where(lax.broadcasted_iota(jnp.int32, (16, LANES), 0) < 3, 1.0, 0.0).astype(BF16)
    zero_blk = jnp.zeros((64, LANES), BF16)

    def fill_const(ref):
        for a in range(2):
            ref[64 * a:64 * a + 64, LANES * (1 - a):LANES * (2 - a)] = zero_blk
            ref[64 * a + 48:64 * a + 64, LANES * a:LANES * (a + 1)] = one_row

    def fill_x(ref, a, val):
        for m in range(3):
            ref[64 * a + 16 * m:64 * a + 16 * m + 16, LANES * a:LANES * (a + 1)] = val

    fill_const(rhs0)
    for a in range(2):
        fill_x(rhs0, a, x_bf)

    row_of = lax.broadcasted_iota(jnp.int32, (8, hidden), 0)

    def terms(p):
        out = []
        for m in range(3):
            out.append(p.astype(BF16))
            if m < 2:
                p = p - out[m].astype(F32)
        return out

    w_out3[...] = jnp.concatenate(terms(w_out_ref[...].astype(F32) * (0.5 / CUBE)), axis=0)

    def prep(pair, w_ref):
        blocks = []
        for a in range(2):
            blocks += terms(w_in32[...] * (CUBE * (1.0 + mods[pair, 0, a:a + 1, :].astype(F32))))
            b = CUBE * mods[pair, 1, a:a + 1, :].astype(F32)
            rows = jnp.zeros((8, hidden), F32)
            for m, q in enumerate(terms(b)):
                rows = jnp.where(row_of == m, q.astype(F32), rows)
            blocks.append(jnp.concatenate([rows, jnp.zeros((8, hidden), F32)], axis=0).astype(BF16))
        w_t = jnp.concatenate(blocks, axis=0).T
        w_ref[...] = w_t
        w_all[pair] = w_t

    def body(a_pair, b_on, c_on, par, rhs=None, nxt=None):
        pre_w, pre_r, act_w, act_r = pres[par], pres[1 - par], acts[1 - par], acts[par]
        total = None
        if a_pair is not None:
            w = w_all.at[a_pair] if rhs is None else wps[par]
            rhs = rhs_all.at[a_pair] if rhs is None else rhs
        if a_pair is not None:
            pre_w[...] = jnp.dot(w[...], rhs[...], preferred_element_type=F32)
        if c_on:
            parts = jnp.dot(w_out3[...], act_r[...], preferred_element_type=F32)
            total = parts[:16] + (parts[16:32] + parts[32:])
        if nxt is not None:
            prep(nxt, wps[1 - par])
        if b_on:
            for c in range(chunks):
                rows = slice(128 * c, 128 * c + 128)
                h = pre_r[rows, :]
                t = jnp.tanh(h * (LIN + h * h))
                act_w[rows, :] = (h + h * t).astype(BF16)
        return total

    def drift_to_x(pair, raw, emit):
        total = jnp.where(pair == 0, 0.0, run_sum[...])
        for a in range(2):
            emit(a, x_own[...] + total)
            total = total + raw[:, LANES * a:LANES * (a + 1)] * steps[pair, a:a + 1, :]
        run_sum[...] = total

    def emit_rhs(pair):
        def emit(a, val):
            stage[pair, a] = val
            fill_x(rhs_all.at[pair], a, val.astype(BF16))
        return emit

    def emit_fix(pair):
        def emit(a, val):
            fix[pair, a] = (val - stage[pair, a]).astype(BF16)
        return emit

    def rot(i):
        return lax.rem(me + i, n_time)

    def wait_mods(lo, count):
        for k in range(count):
            mod_copy(rot(lo + k), me).wait_recv()

    def block(lo, hi, f):
        @pl.loop(lo // 2, hi // 2, unroll=True)
        def _(kk):
            for par in range(2):
                f(2 * kk + par, par)

    def first(t, par, b_on=True, c_on=True, nxt=True):
        raw = body(rot(t), b_on, c_on, par, rhs0, rot(t + 1) if nxt else None)
        if c_on:
            raw_all[rot(t - 2)] = raw
        fill_const(rhs_all.at[t])

    prep(me, wps[0])
    pl.semaphore_wait(barrier, n_time - 1)

    @pl.loop(1, 3 * UNROLL + 1)
    def _(r):
        send_mods(r)

    wait_mods(1, 2)
    first(0, 0, False, False)
    first(1, 1, True, False)
    wait_mods(3, UNROLL - 2)
    block(2, UNROLL, first)

    spread = -(-(n_time - 1) // (n_time // UNROLL - 2))

    @pl.loop(1, n_time // UNROLL - 1)
    def _(i):
        for k in range(UNROLL):
            r = UNROLL * (i + 2) + 1 + k

            @pl.when(r < n_time)
            def _():
                send_mods(r)

        @pl.loop(0, spread)
        def _(k):
            r = (i - 1) * spread + k + 1

            @pl.when(r < n_time)
            def _():
                step_copy(lax.rem(me + r, n_time)).start()
        wait_mods(UNROLL * i + 1, UNROLL)
        block(0, UNROLL, lambda k, par: first(UNROLL * i + k, par))

    wait_mods(n_time - UNROLL + 1, UNROLL - 1)
    block(n_time - UNROLL, n_time - 2, first)
    first(n_time - 2, 0)
    first(n_time - 1, 1, nxt=False)
    raw_all[rot(n_time - 2)] = body(None, True, True, 0)
    raw_all[rot(n_time - 1)] = body(None, False, True, 1)

    others = pl.ds(0, n_time - 1)
    own_step.wait()
    pltpu.make_async_copy(steps.at[others], steps.at[others], step_recv).wait()

    @pl.loop(0, n_time // 2 - 1)
    def _(i):
        for k in range(2):
            drift_to_x(2 * i + k, raw_all[2 * i + k], emit_rhs(2 * i + k))

    def finish_block(i):
        @pl.loop(0, UNROLL, unroll=True)
        def _(k):
            pair = lax.rem(UNROLL * i + k - 2 + n_time, n_time)
            drift_to_x(pair, raw_blk[k], emit_rhs(pair))

    per = n_time // UNROLL
    base_from = (SWEEPS - 3) * n_time

    def mid(k, par, t=None):
        raw_blk[k] = body(k if t is None else t, True, True, par)

    for k in range(2):
        raw_blk[k] = raw_all[n_time - 2 + k]
        body(k, k >= 1, False, k)
    block(2, UNROLL, mid)

    @pl.loop(1, (SWEEPS - 2) * per)
    def _(i):
        for k in range(UNROLL):
            step = UNROLL * (i - 2) + k - 2

            @pl.when(step >= base_from)
            def _():
                send_base(step - base_from)
        finish_block(i - 1)
        block(0, UNROLL, lambda k, par: mid(k, par, lax.rem(UNROLL * i + k, n_time)))

    @pl.loop(0, UNROLL)
    def _(k):
        send_base(n_time - 2 * UNROLL - 2 + k)
    finish_block((SWEEPS - 2) * per - 1)
    for k in range(2):
        drift_to_x(n_time - 2 + k, body(k, True, True, k), emit_rhs(n_time - 2 + k))

    def late(t, par):
        drift_to_x(t - 2, body(t, True, True, par), emit_fix(t - 2))

    block(2, UNROLL, late)

    @pl.loop(0, UNROLL + 2)
    def _(k):
        send_base(n_time - UNROLL - 2 + k)

    @pl.loop(0, UNROLL - 2)
    def _(k):
        send_fix(k)

    @pl.loop(1, per - 1)
    def _(i):
        for k in range(UNROLL):
            @pl.when(i > 1)
            def _():
                send_fix(UNROLL * (i - 1) + k - 2)
        block(0, UNROLL, lambda k, par: late(UNROLL * i + k, par))

    @pl.loop(0, UNROLL)
    def _(k):
        send_fix(n_time - 2 * UNROLL - 2 + k)

    @pl.loop(n_time // 2 - UNROLL // 2, n_time // 2)
    def _(i):
        for par in range(2):
            late(2 * i + par, par)
        for par in range(2):
            send_fix(2 * i + par - 2)

    drift_to_x(n_time - 2, body(None, True, True, 0), emit_fix(n_time - 2))
    send_fix(n_time - 2)
    drift_to_x(n_time - 1, body(None, False, True, 1), emit_fix(n_time - 1))
    send_fix(n_time - 1)

    own = [
        pltpu.make_async_copy(stage.at[me], out_ref.at[:, samp, :, pl.ds(off, LANES)], local_sem.at[0]),
        pltpu.make_async_copy(fix.at[me], fix_ref.at[:, samp, :, pl.ds(off, LANES)], local_sem.at[1]),
    ]
    for c in own:
        c.start()
    for ref, sem in ((mods, mod_send), (steps, step_send), (stage, out_send), (fix, fix_send), (stage, out_recv), (fix, fix_recv)):
        pltpu.make_async_copy(ref.at[others], ref.at[others], sem).wait()
    for c in own:
        c.wait()


def solution(mesh):
    n_time = mesh.shape["time"]

    def local_run(x_init, w_in, w_out, mod_scale, mod_shift, step_size):
        x_t = jnp.transpose(x_init, (0, 2, 1))
        chan, hidden = w_in.shape
        batch, tokens = x_init.shape[0], x_init.shape[1]
        vmem = pl.BlockSpec(memory_space=pltpu.VMEM)
        base, fix = pl.pallas_call(
            functools.partial(kernel, n_time),
            out_shape=[jax.ShapeDtypeStruct((2, batch, chan, tokens), t) for t in (F32, BF16)],
            in_specs=[pl.BlockSpec(memory_space=pl.ANY), vmem, vmem, vmem, vmem,
                      pl.BlockSpec(memory_space=pltpu.SMEM)],
            out_specs=[vmem, vmem],
            scratch_shapes=[
                pltpu.VMEM((chan, LANES), F32),
                pltpu.VMEM((chan, hidden), F32),
                pltpu.VMEM((n_time, 2, 2, hidden), BF16),
                pltpu.VMEM((n_time, 2, LANES), F32),
                pltpu.VMEM((2, LANES), F32),
                pltpu.VMEM((n_time, hidden, 128), BF16),
                pltpu.VMEM((128, 2 * LANES), BF16),
                pltpu.VMEM((n_time, 128, 2 * LANES), BF16),
                pltpu.VMEM((n_time, chan, 2 * LANES), F32),
                pltpu.VMEM((UNROLL, chan, 2 * LANES), F32),
                pltpu.VMEM((n_time, 2, chan, LANES), F32),
                pltpu.VMEM((n_time, 2, chan, LANES), BF16),
                pltpu.VMEM((chan, LANES), F32),
                pltpu.VMEM((hidden, 2 * LANES), F32),
                pltpu.VMEM((hidden, 2 * LANES), F32),
                pltpu.VMEM((hidden, 2 * LANES), BF16),
                pltpu.VMEM((hidden, 2 * LANES), BF16),
                pltpu.VMEM((hidden, 128), BF16),
                pltpu.VMEM((hidden, 128), BF16),
                pltpu.VMEM((3 * chan, hidden), BF16),
                pltpu.SemaphoreType.DMA((3,)),
                pltpu.SemaphoreType.DMA,
                pltpu.SemaphoreType.DMA((n_time,)),
                pltpu.SemaphoreType.DMA,
                pltpu.SemaphoreType.DMA,
                pltpu.SemaphoreType.DMA,
                pltpu.SemaphoreType.DMA,
                pltpu.SemaphoreType.DMA,
                pltpu.SemaphoreType.DMA,
            ],
            compiler_params=pltpu.CompilerParams(collective_id=0, has_side_effects=True, vmem_limit_bytes=58 * 1024 * 1024),
            name="picard",
        )(x_t, w_in, w_out.T, mod_scale, mod_shift, step_size)
        return jnp.transpose(base + fix.astype(F32), (0, 1, 3, 2))

    return jax.shard_map(
        local_run,
        mesh=mesh,
        in_specs=(P(("part", "data"), None, None), P(None, None), P(None, None), P("time", None), P("time", None), P("time")),
        out_specs=P("time", ("part", "data"), None, None),
        check_vma=False,
    )
```

```python
import functools

import jax
import jax.numpy as jnp
from jax import lax
from jax.experimental import pallas as pl
from jax.experimental.pallas import tpu as pltpu
from jax.sharding import PartitionSpec as P

SWEEPS = 4
UNROLL = 8
ROOT = 0.7978845608028654
CUBE = (ROOT * 0.044715) ** (1.0 / 3.0)
LIN = ROOT / CUBE
LANES = 128
F32 = jnp.float32
BF16 = jnp.bfloat16


def kernel(n_time, x_hbm, w_in_ref, w_out_ref, scale_ref, shift_ref, step_ref, out_ref, fix_ref,
           x_own, w_in32, mods, steps, step_own, w_all, rhs0, rhs_all, raw_all, raw_blk, stage, fix, run_sum,
           pre0, pre1, act0, act1, wp0, wp1, w_out3,
           local_sem, mod_send, mod_recv, step_send, step_recv, out_send, out_recv, fix_send, fix_recv):
    hidden = w_in_ref.shape[1]
    chunks = hidden // 128
    tiles = x_hbm.shape[2] // LANES
    me = lax.axis_index("time")
    samp = me // tiles
    off = pl.multiple_of(lax.rem(me, tiles) * LANES, LANES)
    pres, acts, wps = (pre0, pre1), (act0, act1), (wp0, wp1)

    barrier = pltpu.get_barrier_semaphore()

    @pl.loop(1, n_time)
    def _(r):
        pl.semaphore_signal(
            barrier, inc=1, device_id={"time": lax.rem(me + r, n_time)}, device_id_type=pl.DeviceIdType.MESH)

    copies = [
        pltpu.make_async_copy(x_hbm.at[samp, :, pl.ds(off, LANES)], x_own, local_sem.at[0]),
        pltpu.make_async_copy(scale_ref, mods.at[me, 0], local_sem.at[1]),
        pltpu.make_async_copy(shift_ref, mods.at[me, 1], local_sem.at[2]),
    ]
    for c in copies:
        c.start()
    for a in range(2):
        step_own[a:a + 1, :] = jnp.full((1, LANES), step_ref[a], F32)
    w_in32[...] = w_in_ref[...].astype(F32)
    for c in copies:
        c.wait()

    def mod_copy(slot, peer):
        return pltpu.make_async_remote_copy(
            src_ref=mods.at[slot], dst_ref=mods.at[slot], send_sem=mod_send, recv_sem=mod_recv.at[slot],
            device_id={"time": peer}, device_id_type=pl.DeviceIdType.MESH)

    def step_copy(peer):
        return pltpu.make_async_remote_copy(
            src_ref=step_own, dst_ref=steps.at[me], send_sem=step_send, recv_sem=step_recv,
            device_id={"time": peer}, device_id_type=pl.DeviceIdType.MESH)

    def send_to(pair, src, dst, send, recv):
        @pl.when(pair != me)
        def _():
            pltpu.make_async_remote_copy(
                src_ref=src.at[pair], dst_ref=dst.at[:, samp, :, pl.ds(off, LANES)], send_sem=send, recv_sem=recv,
                device_id={"time": pair}, device_id_type=pl.DeviceIdType.MESH).start()

    def send_base(pair):
        send_to(pair, stage, out_ref, out_send, out_recv)

    def send_fix(pair):
        send_to(pair, fix, fix_ref, fix_send, fix_recv)

    own_step = pltpu.make_async_copy(step_own, steps.at[me], local_sem.at[0])
    own_step.start()

    def send_mods(r):
        mod_copy(me, lax.rem(me + n_time - r, n_time)).start()

    x_bf = x_own[...].astype(BF16)
    one_row = jnp.where(lax.broadcasted_iota(jnp.int32, (16, LANES), 0) < 3, 1.0, 0.0).astype(BF16)
    zero_blk = jnp.zeros((64, LANES), BF16)

    def fill_const(ref):
        for a in range(2):
            ref[64 * a:64 * a + 64, LANES * (1 - a):LANES * (2 - a)] = zero_blk
            ref[64 * a + 48:64 * a + 64, LANES * a:LANES * (a + 1)] = one_row

    def fill_x(ref, a, val):
        for m in range(3):
            ref[64 * a + 16 * m:64 * a + 16 * m + 16, LANES * a:LANES * (a + 1)] = val

    fill_const(rhs0)
    for a in range(2):
        fill_x(rhs0, a, x_bf)

    row_of = lax.broadcasted_iota(jnp.int32, (8, hidden), 0)

    def terms(p):
        out = []
        for m in range(3):
            out.append(p.astype(BF16))
            if m < 2:
                p = p - out[m].astype(F32)
        return out

    w_out3[...] = jnp.concatenate(terms(w_out_ref[...].astype(F32) * (0.5 / CUBE)), axis=0)

    def prep(pair, w_ref):
        blocks = []
        for a in range(2):
            blocks += terms(w_in32[...] * (CUBE * (1.0 + mods[pair, 0, a:a + 1, :].astype(F32))))
            b = CUBE * mods[pair, 1, a:a + 1, :].astype(F32)
            rows = jnp.zeros((8, hidden), F32)
            for m, q in enumerate(terms(b)):
                rows = jnp.where(row_of == m, q.astype(F32), rows)
            blocks.append(jnp.concatenate([rows, jnp.zeros((8, hidden), F32)], axis=0).astype(BF16))
        w_t = jnp.concatenate(blocks, axis=0).T
        w_ref[...] = w_t
        w_all[pair] = w_t

    def body(a_pair, b_on, c_on, par, rhs=None, nxt=None):
        pre_w, pre_r, act_w, act_r = pres[par], pres[1 - par], acts[1 - par], acts[par]
        total = None
        if a_pair is not None:
            w = w_all.at[a_pair] if rhs is None else wps[par]
            rhs = rhs_all.at[a_pair] if rhs is None else rhs
        if a_pair is not None:
            pre_w[...] = jnp.dot(w[...], rhs[...], preferred_element_type=F32)
        if c_on:
            parts = jnp.dot(w_out3[...], act_r[...], preferred_element_type=F32)
            total = parts[:16] + (parts[16:32] + parts[32:])
        if nxt is not None:
            prep(nxt, wps[1 - par])
        if b_on:
            for c in range(chunks):
                rows = slice(128 * c, 128 * c + 128)
                h = pre_r[rows, :]
                t = jnp.tanh(h * (LIN + h * h))
                act_w[rows, :] = (h + h * t).astype(BF16)
        return total

    def drift_to_x(pair, raw, emit):
        total = jnp.where(pair == 0, 0.0, run_sum[...])
        for a in range(2):
            emit(a, x_own[...] + total)
            total = total + raw[:, LANES * a:LANES * (a + 1)] * steps[pair, a:a + 1, :]
        run_sum[...] = total

    def emit_rhs(pair):
        def emit(a, val):
            stage[pair, a] = val
            fill_x(rhs_all.at[pair], a, val.astype(BF16))
        return emit

    def emit_fix(pair):
        def emit(a, val):
            fix[pair, a] = (val - stage[pair, a]).astype(BF16)
        return emit

    def rot(i):
        return lax.rem(me + i, n_time)

    def wait_mods(lo, count):
        for k in range(count):
            mod_copy(rot(lo + k), me).wait_recv()

    def block(lo, hi, f):
        @pl.loop(lo // 2, hi // 2, unroll=True)
        def _(kk):
            for par in range(2):
                f(2 * kk + par, par)

    def first(t, par, b_on=True, c_on=True, nxt=True):
        raw = body(rot(t), b_on, c_on, par, rhs0, rot(t + 1) if nxt else None)
        if c_on:
            raw_all[rot(t - 2)] = raw
        fill_const(rhs_all.at[t])

    prep(me, wps[0])
    pl.semaphore_wait(barrier, n_time - 1)

    @pl.loop(1, 3 * UNROLL + 1)
    def _(r):
        send_mods(r)

    wait_mods(1, 2)
    first(0, 0, False, False)
    first(1, 1, True, False)

    @pl.loop(1, UNROLL // 2)
    def _(i):
        wait_mods(2 * i + 1, 2)
        for par in range(2):
            first(2 * i + par, par)

    spread = -(-(n_time - 1) // (n_time // UNROLL - 2))

    @pl.loop(1, n_time // UNROLL - 1)
    def _(i):
        for k in range(UNROLL):
            r = UNROLL * (i + 2) + 1 + k

            @pl.when(r < n_time)
            def _():
                send_mods(r)

        @pl.loop(0, spread)
        def _(k):
            r = (i - 1) * spread + k + 1

            @pl.when(r < n_time)
            def _():
                step_copy(lax.rem(me + r, n_time)).start()
        wait_mods(UNROLL * i + 1, UNROLL)
        block(0, UNROLL, lambda k, par: first(UNROLL * i + k, par))

    wait_mods(n_time - UNROLL + 1, UNROLL - 1)
    block(n_time - UNROLL, n_time - 2, first)
    first(n_time - 2, 0)
    first(n_time - 1, 1, nxt=False)
    raw_all[rot(n_time - 2)] = body(None, True, True, 0)
    raw_all[rot(n_time - 1)] = body(None, False, True, 1)

    others = pl.ds(0, n_time - 1)
    own_step.wait()
    pltpu.make_async_copy(steps.at[others], steps.at[others], step_recv).wait()

    @pl.loop(0, n_time // 2 - 1)
    def _(i):
        for k in range(2):
            drift_to_x(2 * i + k, raw_all[2 * i + k], emit_rhs(2 * i + k))

    def finish_block(i):
        @pl.loop(0, UNROLL, unroll=True)
        def _(k):
            pair = lax.rem(UNROLL * i + k - 2 + n_time, n_time)
            drift_to_x(pair, raw_blk[k], emit_rhs(pair))

    per = n_time // UNROLL
    base_from = (SWEEPS - 3) * n_time

    def mid(k, par, t=None):
        raw_blk[k] = body(k if t is None else t, True, True, par)

    for k in range(2):
        raw_blk[k] = raw_all[n_time - 2 + k]
        body(k, k >= 1, False, k)
    block(2, UNROLL, mid)

    @pl.loop(1, (SWEEPS - 2) * per)
    def _(i):
        for k in range(UNROLL):
            step = UNROLL * (i - 2) + k - 2

            @pl.when(step >= base_from)
            def _():
                send_base(step - base_from)
        finish_block(i - 1)
        block(0, UNROLL, lambda k, par: mid(k, par, lax.rem(UNROLL * i + k, n_time)))

    @pl.loop(0, UNROLL)
    def _(k):
        send_base(n_time - 2 * UNROLL - 2 + k)
    finish_block((SWEEPS - 2) * per - 1)
    for k in range(2):
        drift_to_x(n_time - 2 + k, body(k, True, True, k), emit_rhs(n_time - 2 + k))

    def late(t, par):
        drift_to_x(t - 2, body(t, True, True, par), emit_fix(t - 2))

    block(2, UNROLL, late)

    @pl.loop(0, UNROLL + 2)
    def _(k):
        send_base(n_time - UNROLL - 2 + k)

    @pl.loop(0, UNROLL - 2)
    def _(k):
        send_fix(k)

    @pl.loop(1, per - 1)
    def _(i):
        for k in range(UNROLL):
            @pl.when(i > 1)
            def _():
                send_fix(UNROLL * (i - 1) + k - 2)
        block(0, UNROLL, lambda k, par: late(UNROLL * i + k, par))

    @pl.loop(0, UNROLL)
    def _(k):
        send_fix(n_time - 2 * UNROLL - 2 + k)

    @pl.loop(n_time // 2 - UNROLL // 2, n_time // 2)
    def _(i):
        for par in range(2):
            late(2 * i + par, par)
        for par in range(2):
            send_fix(2 * i + par - 2)

    drift_to_x(n_time - 2, body(None, True, True, 0), emit_fix(n_time - 2))
    send_fix(n_time - 2)
    drift_to_x(n_time - 1, body(None, False, True, 1), emit_fix(n_time - 1))
    send_fix(n_time - 1)

    own = [
        pltpu.make_async_copy(stage.at[me], out_ref.at[:, samp, :, pl.ds(off, LANES)], local_sem.at[0]),
        pltpu.make_async_copy(fix.at[me], fix_ref.at[:, samp, :, pl.ds(off, LANES)], local_sem.at[1]),
    ]
    for c in own:
        c.start()
    for ref, sem in ((mods, mod_send), (steps, step_send), (stage, out_send), (fix, fix_send), (stage, out_recv), (fix, fix_recv)):
        pltpu.make_async_copy(ref.at[others], ref.at[others], sem).wait()
    for c in own:
        c.wait()


def solution(mesh):
    n_time = mesh.shape["time"]

    def local_run(x_init, w_in, w_out, mod_scale, mod_shift, step_size):
        x_t = jnp.transpose(x_init, (0, 2, 1))
        chan, hidden = w_in.shape
        batch, tokens = x_init.shape[0], x_init.shape[1]
        vmem = pl.BlockSpec(memory_space=pltpu.VMEM)
        base, fix = pl.pallas_call(
            functools.partial(kernel, n_time),
            out_shape=[jax.ShapeDtypeStruct((2, batch, chan, tokens), t) for t in (F32, BF16)],
            in_specs=[pl.BlockSpec(memory_space=pl.ANY), vmem, vmem, vmem, vmem,
                      pl.BlockSpec(memory_space=pltpu.SMEM)],
            out_specs=[pl.BlockSpec(memory_space=pl.ANY)] * 2,
            scratch_shapes=[
                pltpu.VMEM((chan, LANES), F32),
                pltpu.VMEM((chan, hidden), F32),
                pltpu.VMEM((n_time, 2, 2, hidden), BF16),
                pltpu.VMEM((n_time, 2, LANES), F32),
                pltpu.VMEM((2, LANES), F32),
                pltpu.VMEM((n_time, hidden, 128), BF16),
                pltpu.VMEM((128, 2 * LANES), BF16),
                pltpu.VMEM((n_time, 128, 2 * LANES), BF16),
                pltpu.VMEM((n_time, chan, 2 * LANES), F32),
                pltpu.VMEM((UNROLL, chan, 2 * LANES), F32),
                pltpu.VMEM((n_time, 2, chan, LANES), F32),
                pltpu.VMEM((n_time, 2, chan, LANES), BF16),
                pltpu.VMEM((chan, LANES), F32),
                pltpu.VMEM((hidden, 2 * LANES), F32),
                pltpu.VMEM((hidden, 2 * LANES), F32),
                pltpu.VMEM((hidden, 2 * LANES), BF16),
                pltpu.VMEM((hidden, 2 * LANES), BF16),
                pltpu.VMEM((hidden, 128), BF16),
                pltpu.VMEM((hidden, 128), BF16),
                pltpu.VMEM((3 * chan, hidden), BF16),
                pltpu.SemaphoreType.DMA((3,)),
                pltpu.SemaphoreType.DMA,
                pltpu.SemaphoreType.DMA((n_time,)),
                pltpu.SemaphoreType.DMA,
                pltpu.SemaphoreType.DMA,
                pltpu.SemaphoreType.DMA,
                pltpu.SemaphoreType.DMA,
                pltpu.SemaphoreType.DMA,
                pltpu.SemaphoreType.DMA,
            ],
            compiler_params=pltpu.CompilerParams(collective_id=0, has_side_effects=True, vmem_limit_bytes=58 * 1024 * 1024),
            name="picard",
        )(x_t, w_in, w_out.T, mod_scale, mod_shift, step_size)
        return jnp.transpose(base + fix.astype(F32), (0, 1, 3, 2))

    return jax.shard_map(
        local_run,
        mesh=mesh,
        in_specs=(P(("part", "data"), None, None), P(None, None), P(None, None), P("time", None), P("time", None), P("time")),
        out_specs=P("time", ("part", "data"), None, None),
        check_vma=False,
    )
```
